1024 devices in a mesh: fsdp: 64 (over y_lo, z), grp: 16 (over y_hi, x, core).
Axes of the slice: x: 4, y: 4 (y_hi: 2, y_lo: 2; y = y_hi * 2 + y_lo), z: 32, core: 2. Of those that a mesh axis runs over, the one named last changes fastest.
Arguments:
- grads: bfloat16 [16, 64, 128, 8192], P('grp', 'fsdp'), may hold values from -16 to 16
- master: float32 [128, 8192], P('fsdp', 'grp'), may hold values from -0.0625 to 0.0625
- moment_one: float32 [128, 8192], P('fsdp', 'grp'), may hold values from -0.2 to 0.2
- moment_two: float32 [128, 8192], P('fsdp', 'grp'), may hold values from 0.0001 to 0.004
Outputs:
- new_master: float32 [128, 8192], P('fsdp', 'grp')
- new_first: float32 [128, 8192], P('fsdp', 'grp')
- new_second: float32 [128, 8192], P('fsdp', 'grp')
- weights: bfloat16 [128, 8192], P('fsdp')
- copy_master: float32 [128, 8192], P('fsdp', 'grp')
- copy_first: float32 [128, 8192], P('fsdp', 'grp')
- copy_second: float32 [128, 8192], P('fsdp', 'grp')
The draws below stay inside these ranges and needn't reach their ends.
All inputs are finite; a program needn't handle non-finite values.
Results may differ from the reference program's by a relative error of at most 0.009.
Values may be sent and summed in bfloat16 or wider, within the bound.
A program may use at most 32 MiB of HBM per device.

```python
import math
import jax
import jax.numpy as jnp
from jax import lax

D = 8192
ROWS = 128
N_FSDP = 64
N_GRP = 16


def with_spikes(values, rng, source, target, blocks, factor):
    owner, partner = [(jnp.arange(values.shape[axis_at]) // (values.shape[axis_at] // blocks)).reshape([-1 if axis == axis_at else 1 for axis in range(values.ndim)]) for axis_at in (source, target)]
    chosen = jax.random.permutation(rng, blocks)[partner]
    strong = (owner == chosen) | (owner == (partner + blocks // 2) % blocks)
    return jnp.where(strong, factor * values, values)


def shard_levels(stream_key, dims, shards, least, high):
    level, own = 1.0, jax.random.fold_in(stream_key, 6)
    for dim, blocks in shards:
        steps = jnp.exp(jax.random.uniform(jax.random.fold_in(own, dim), (blocks,), jnp.float32, least / len(shards), high / len(shards)))
        level = level * jnp.repeat(steps, dims[dim] // blocks).reshape([-1 if axis == dim else 1 for axis in range(len(dims))])
    return level


def bell_draw(key, shape, spread, limit, shards=(), dtype=jnp.bfloat16):
    factor_of = shard_levels(key, shape, shards, -0.22, 0.18) if shards else 1.0
    array = jax.random.normal(key, shape, jnp.float32) * spread * factor_of
    return jnp.minimum(jnp.maximum(array, -limit), limit).astype(dtype)


def noise_with(rng, shape, width, limit, shards, heavy, dtype=jnp.bfloat16):
    entries = width * jax.random.normal(rng, shape, jnp.float32)
    if shards:
        entries = entries * shard_levels(rng, shape, shards, -0.22, 0.18)
    return jnp.clip(with_spikes(entries, jax.random.fold_in(rng, 3), *heavy), -limit, limit).astype(dtype)


def setup_inputs(seed: int = 0) -> dict:
    keys = jax.random.split(jax.random.key(seed), 5)
    return {
        "grads": noise_with(keys[0], (N_GRP, N_FSDP, ROWS, D), 1.0, 16.0, ((0, 16), (1, 64)), (1, 2, 64, 4.0)),
        "master": bell_draw(keys[1], (ROWS, D), D ** -0.5, 0.0625, ((0, 64), (1, 16)), jnp.float32),
        "moment_one": bell_draw(keys[2], (ROWS, D), 0.03, 0.2, ((0, 64), (1, 16)), jnp.float32),
        "moment_two": jnp.clip(jnp.exp(math.log(0.004) - 3.6888795 * jax.random.uniform(keys[3], (ROWS, D), jnp.float32) ** shard_levels(keys[3], (ROWS, D), ((0, 64), (1, 16)), -0.2, 0.2)), 0.0001, 0.004),
    }


beta_one = 0.9
beta_two = 0.95
learn_rate = 0.01
decay_rate = 0.1
epsilon = 1e-08
step_count = 100

def accumulate(carry, block):
    return (carry + lax.optimization_barrier(jnp.sum(block.astype(jnp.float32), axis=0)), None)

def reference(grads, master, moment_one, moment_two):
    summed, _ = lax.scan(accumulate, jnp.zeros((ROWS, D), jnp.float32), grads)
    gradient = summed / (N_GRP * N_FSDP)
    new_first = beta_one * moment_one + (1.0 - beta_one) * gradient
    new_second = beta_two * moment_two + (1.0 - beta_two) * gradient * gradient
    first_hat = new_first / (1.0 - beta_one ** step_count)
    second_hat = new_second / (1.0 - beta_two ** step_count)
    new_master = master - learn_rate * (first_hat / (jnp.sqrt(second_hat) + epsilon) + decay_rate * master)
    weights = new_master.astype(jnp.bfloat16)
    offset = D // N_GRP
    copy_master = jnp.roll(new_master, offset, axis=1)
    copy_first = jnp.roll(new_first, offset, axis=1)
    copy_second = jnp.roll(new_second, offset, axis=1)
    return (new_master, new_first, new_second, weights, copy_master, copy_first, copy_second)
```

```python
import functools

import jax
import jax.numpy as jnp
from jax import lax
from jax.experimental import pallas as pl
from jax.experimental.pallas import tpu as pltpu
from jax.sharding import PartitionSpec as P

MESH = pl.DeviceIdType.MESH

beta_one = 0.9
beta_two = 0.95
learn_rate = 0.01
decay_rate = 0.1
epsilon = 1e-08
step_count = 100

N_X, N_Y, N_Y_LO, N_CORE = 4, 4, 2, 2
LANES = 128


def add(*terms):
    total = terms[0].astype(jnp.float32)
    for term in terms[1:]:
        total = total + term.astype(jnp.float32)
    return total


def kernel(
    n_z, n_grp, n_fsdp,
    grads, master, first, second,
    new_master, new_first, new_second, weights, copy_master, copy_first, copy_second,
    own, other, one_up, one_down, two_up, two_down,
    part, late_one_up, late_one_down, late_two_up, late_two_down,
    flat, leaving, arriving, total,
    own_sem, other_sem, other_sent, ring_sem, ring_sent, late_sem, late_sent,
    far_sem, far_sent, weights_sem, weights_sent, copy_sem, copy_sent, known_sem,
):
    f, g = lax.axis_index("fsdp"), lax.axis_index("grp")
    z, y_lo = lax.rem(f, n_z), f // n_z
    core, x, y_hi = lax.rem(g, N_CORE), lax.rem(g // N_CORE, N_X), g // (N_CORE * N_X)
    y = y_hi * N_Y_LO + y_lo
    half_rows, width = own.shape[-2:]

    def device(dx=0, dy=0, dz=0, flip=False):
        to_x, to_y = lax.rem(x + dx + N_X, N_X), lax.rem(y + dy + N_Y, N_Y)
        to_z = lax.rem(z + dz + n_z, n_z)
        to_core = 1 - core if flip else core
        return (
            lax.rem(to_y, N_Y_LO) * n_z + to_z,
            ((to_y // N_Y_LO) * N_X + to_x) * N_CORE + to_core,
        )

    def send(source, target, sent, received, to):
        copy = pltpu.make_async_remote_copy(
            src_ref=source, dst_ref=target, send_sem=sent, recv_sem=received,
            device_id=to, device_id_type=MESH,
        )
        copy.start()

    def await_bytes(ref, sem):
        pltpu.make_async_copy(ref, ref, sem).wait()

    def tell(sem, to):
        pl.semaphore_signal(sem, inc=1, device_id=to, device_id_type=MESH)

    def block(a, k, j, of_core):
        dx, dy = (k, j) if a == 0 else (j, k)
        to_x, to_y = lax.rem(x + dx, N_X), lax.rem(y + dy, N_Y)
        owner = ((to_y // N_Y_LO) * N_X + to_x) * N_CORE + of_core
        column = pl.multiple_of(owner * width, width)
        return grads.at[
            lax.rem(to_y, N_Y_LO), pl.ds(a * half_rows, half_rows), pl.ds(column, width)
        ]

    order = (2, 1, 3, 0)
    near = [
        device(flip=True), device(dx=1), device(dx=-1), device(dy=1), device(dy=-1),
        device(dz=1), device(dz=-1),
    ]
    barrier = pltpu.get_barrier_semaphore()
    for to in near:
        tell(barrier, to)
    for k in order:
        for a in range(2):
            for j in range(4):
                pltpu.make_async_copy(
                    block(a, k, j, core), own.at[a, k, j], own_sem.at[a, k]
                ).start()
    pl.semaphore_wait(barrier, len(near))

    for k in order:
        for a in range(2):
            for j in range(4):
                send(
                    block(a, k, j, 1 - core), other.at[a, k, j],
                    other_sent, other_sem.at[a, k], near[0],
                )

    strides = [1 << i for i in range(known_sem.shape[0])]

    def tell_far(i):
        for step in (strides[i], -strides[i]):
            tell(known_sem.at[i], device(dz=step))

    def await_far(i):
        pl.semaphore_wait(known_sem.at[i], 2)

    up = (device(dx=1), device(dy=1))
    down = (device(dx=-1), device(dy=-1))

    def both_cores(a, k):
        await_bytes(own.at[a, k], own_sem.at[a, k])
        await_bytes(other.at[a, k], other_sem.at[a, k])
        own[a, k] = add(own[a, k], other[a, k]).astype(own.dtype)

    tell_far(0)
    await_far(0)
    tell_far(1)
    for a in range(2):
        both_cores(a, 2)
        send(own.at[a, 2, 0:2], one_up.at[a], ring_sent.at[a, 0], ring_sem.at[a, 0], up[a])
        send(own.at[a, 2, 2:4], one_down.at[a], ring_sent.at[a, 1], ring_sem.at[a, 1], down[a])
    await_far(1)
    tell_far(2)
    for a in range(2):
        both_cores(a, 1)
        send(own.at[a, 1, 2:4], two_up.at[a, 2:4], ring_sent.at[a, 2], ring_sem.at[a, 2], up[a])
        both_cores(a, 3)
        send(own.at[a, 3, 0:2], two_down.at[a, 0:2], ring_sent.at[a, 3], ring_sem.at[a, 3], down[a])
    for a in range(2):
        await_bytes(one_up.at[a], ring_sem.at[a, 0])
        own[a, 1, 0:2] = add(own[a, 1, 0:2], one_up[a]).astype(own.dtype)
        send(own.at[a, 1, 0:2], two_up.at[a, 0:2], ring_sent.at[a, 4], ring_sem.at[a, 4], up[a])
        await_bytes(one_down.at[a], ring_sem.at[a, 1])
        own[a, 3, 2:4] = add(own[a, 3, 2:4], one_down[a]).astype(own.dtype)
        send(own.at[a, 3, 2:4], two_down.at[a, 2:4], ring_sent.at[a, 5], ring_sem.at[a, 5], down[a])
    await_far(2)
    tell_far(3)
    for a in range(2):
        both_cores(a, 0)
    for a in range(2):
        await_bytes(two_up.at[a, 2:4], ring_sem.at[a, 2])
        await_bytes(two_down.at[a, 0:2], ring_sem.at[a, 3])
        await_bytes(two_up.at[a, 0:2], ring_sem.at[a, 4])
        await_bytes(two_down.at[a, 2:4], ring_sem.at[a, 5])
        part[a, 2] = add(own[a, 0, 2], two_up[a, 2], two_down[a, 2]).astype(part.dtype)
        mid = half_rows // 2
        send(part.at[a, 2, 0:mid], late_one_up.at[a], late_sent.at[a, 0], late_sem.at[a, 0], up[1 - a])
        send(part.at[a, 2, mid:], late_one_down.at[a], late_sent.at[a, 1], late_sem.at[a, 1], down[1 - a])
        for j in (1, 3, 0):
            part[a, j] = add(own[a, 0, j], two_up[a, j], two_down[a, j]).astype(part.dtype)
        send(part.at[a, 1, mid:], late_two_up.at[a, mid:], late_sent.at[a, 2], late_sem.at[a, 2], up[1 - a])
        send(part.at[a, 3, 0:mid], late_two_down.at[a, 0:mid], late_sent.at[a, 3], late_sem.at[a, 3], down[1 - a])
    for a in range(2):
        await_bytes(late_one_up.at[a], late_sem.at[a, 0])
        part[a, 1, 0:mid] = add(part[a, 1, 0:mid], late_one_up[a]).astype(part.dtype)
        send(part.at[a, 1, 0:mid], late_two_up.at[a, 0:mid], late_sent.at[a, 4], late_sem.at[a, 4], up[1 - a])
        await_bytes(late_one_down.at[a], late_sem.at[a, 1])
        part[a, 3, mid:] = add(part[a, 3, mid:], late_one_down[a]).astype(part.dtype)
        send(part.at[a, 3, mid:], late_two_down.at[a, mid:], late_sent.at[a, 5], late_sem.at[a, 5], down[1 - a])
    pieces = n_z // 2
    for a in range(2):
        await_bytes(late_two_up.at[a, mid:], late_sem.at[a, 2])
        await_bytes(late_two_down.at[a, 0:mid], late_sem.at[a, 3])
        await_bytes(late_two_up.at[a, 0:mid], late_sem.at[a, 4])
        await_bytes(late_two_down.at[a, mid:], late_sem.at[a, 5])
        plane = add(part[a, 0], late_two_up[a], late_two_down[a])
        for t in range(width // LANES):
            flat[a, pl.ds(t, half_rows, stride=width // LANES), :] = plane[:, t * LANES:(t + 1) * LANES]
        leaving[a * pieces:(a + 1) * pieces] = (
            flat[a].reshape(pieces, *leaving.shape[1:]).astype(leaving.dtype)
        )
    await_far(3)
    far = [n_z // 2]
    for d in range(n_z // 2 - 1, 0, -1):
        far += [d, n_z - d]
    for d in far:
        to_z = lax.rem(z + d, n_z)
        send(leaving.at[to_z], arriving.at[d - 1], far_sent, far_sem, device(dz=d))

    await_bytes(arriving, far_sem)
    total[...] = add(leaving[z], *[arriving[d] for d in range(n_z - 1)])

    scale = 1.0 / (n_grp * n_fsdp)
    for t in range(width // LANES):
        at = slice(t * LANES, (t + 1) * LANES)
        gradient = total[pl.ds(t, 2, stride=width // LANES), :] * scale
        one = beta_one * first[:, at] + (1.0 - beta_one) * gradient
        two = beta_two * second[:, at] + (1.0 - beta_two) * gradient * gradient
        one_hat = one / (1.0 - beta_one**step_count)
        two_hat = two / (1.0 - beta_two**step_count)
        old = master[:, at]
        new = old - learn_rate * (one_hat / (jnp.sqrt(two_hat) + epsilon) + decay_rate * old)
        new_master[:, at] = new
        new_first[:, at] = one
        new_second[:, at] = two
    mine = pl.ds(pl.multiple_of(g * width, width), width)
    weights[:, mine] = new_master[...].astype(weights.dtype)
    after = (f, lax.rem(g + 1, n_grp))
    for i in range(n_grp - 1, 0, -1):
        to = lax.rem(g + i, n_grp)
        send(weights.at[:, mine], weights.at[:, mine], weights_sent.at[i - 1], weights_sem.at[i - 1], (f, to))
    for i, (new, copied) in enumerate(
        ((new_master, copy_master), (new_first, copy_first), (new_second, copy_second))
    ):
        send(new, copied, copy_sent.at[i], copy_sem.at[i], after)

    await_bytes(other, other_sent)
    for a in range(2):
        for i, ref in enumerate((one_up.at[a], one_down.at[a], one_up.at[a], one_up.at[a], one_up.at[a], one_up.at[a])):
            await_bytes(ref, ring_sent.at[a, i])
        for i in range(6):
            await_bytes(late_one_up.at[a], late_sent.at[a, i])
    await_bytes(arriving, far_sent)
    for i in range(1, n_grp):
        source = lax.rem(g - i + n_grp, n_grp)
        theirs = pl.ds(pl.multiple_of(source * width, width), width)
        await_bytes(weights.at[:, theirs], weights_sem.at[i - 1])
        await_bytes(weights.at[:, mine], weights_sent.at[i - 1])
    for i, (new, copied) in enumerate(
        ((new_master, copy_master), (new_first, copy_first), (new_second, copy_second))
    ):
        await_bytes(copied, copy_sem.at[i])
        await_bytes(new, copy_sent.at[i])


def shards(n_fsdp, n_grp, grads, master, moment_one, moment_two):
    rows, columns = grads.shape[2:]
    n_z = n_fsdp // N_Y_LO
    width = columns // n_grp
    half_rows = rows // (2 * N_Y_LO)
    mid = half_rows // 2
    piece = (rows // n_fsdp) * width // LANES
    vmem = pl.BlockSpec(memory_space=pltpu.VMEM)
    small = jax.ShapeDtypeStruct(master.shape, jnp.float32)
    wide = jax.ShapeDtypeStruct((master.shape[0], columns), jnp.bfloat16)
    bf16, f32, dma = jnp.bfloat16, jnp.float32, pltpu.SemaphoreType.DMA
    return pl.pallas_call(
        functools.partial(kernel, n_z, n_grp, n_fsdp),
        out_shape=(small, small, small, wide, small, small, small),
        in_specs=[pl.BlockSpec(memory_space=pl.ANY), vmem, vmem, vmem],
        out_specs=[vmem] * 7,
        scratch_shapes=[
            pltpu.VMEM((2, 4, 4, half_rows, width), bf16),
            pltpu.VMEM((2, 4, 4, half_rows, width), bf16),
            pltpu.VMEM((2, 2, half_rows, width), bf16),
            pltpu.VMEM((2, 2, half_rows, width), bf16),
            pltpu.VMEM((2, 4, half_rows, width), bf16),
            pltpu.VMEM((2, 4, half_rows, width), bf16),
            pltpu.VMEM((2, 4, half_rows, width), bf16),
            pltpu.VMEM((2, mid, width), bf16),
            pltpu.VMEM((2, mid, width), bf16),
            pltpu.VMEM((2, half_rows, width), bf16),
            pltpu.VMEM((2, half_rows, width), bf16),
            pltpu.VMEM((2, half_rows * width // LANES, LANES), f32),
            pltpu.VMEM((n_z, piece, LANES), bf16),
            pltpu.VMEM((n_z - 1, piece, LANES), bf16),
            pltpu.VMEM((piece, LANES), f32),
            dma((2, 4)), dma((2, 4)), dma,
            dma((2, 6)), dma((2, 6)), dma((2, 6)), dma((2, 6)),
            dma, dma,
            dma((n_grp - 1,)), dma((n_grp - 1,)), dma((3,)), dma((3,)),
            pltpu.SemaphoreType.REGULAR((n_z.bit_length() - 2,)),
        ],
        compiler_params=pltpu.CompilerParams(
            collective_id=0, has_side_effects=True, vmem_limit_bytes=16 << 20
        ),
        name="step",
    )(grads.reshape(N_Y_LO, rows // N_Y_LO, columns), master, moment_one, moment_two)


def solution(mesh):
    return jax.shard_map(
        functools.partial(shards, mesh.shape["fsdp"], mesh.shape["grp"]),
        mesh=mesh,
        in_specs=(P("grp", "fsdp", None, None), P("fsdp", "grp"), P("fsdp", "grp"), P("fsdp", "grp")),
        out_specs=(
            P("fsdp", "grp"), P("fsdp", "grp"), P("fsdp", "grp"), P("fsdp", None),
            P("fsdp", "grp"), P("fsdp", "grp"), P("fsdp", "grp"),
        ),
        check_vma=False,
    )
```

```python
import functools

import jax
import jax.numpy as jnp
from jax import lax
from jax.experimental import pallas as pl
from jax.experimental.pallas import tpu as pltpu
from jax.sharding import PartitionSpec as P

MESH = pl.DeviceIdType.MESH

beta_one = 0.9
beta_two = 0.95
learn_rate = 0.01
decay_rate = 0.1
epsilon = 1e-08
step_count = 100

N_X, N_Y, N_Y_LO, N_Y_HI, N_CORE = 4, 4, 2, 2, 2
LANES = 128
CHUNK_ROWS = 8
ORDER = (
    ("X", 0), ("E", 0), ("X", 1), ("X", 2), ("X", 3), ("X", 4), ("X", 5), ("X", 6), ("X", 7), ("E", 1), ("W", 0), ("E", 2),
    ("Q", 0), ("W", 1), ("E", 3), ("Q", 1), ("E", 4), ("Z", 0), ("W", 2), ("E", 5), ("Q", 2), ("E", 6), ("Z", 1), ("Q", 3), ("E", 7), ("Q", 4),
    ("W", 3), ("Z", 2), ("Q", 5), ("Z", 3), ("Q", 6), ("Z", 4), ("Q", 7), ("Z", 5), ("Z", 6), ("Z", 7),
)
GREETERS = 8


def add(*terms):
    total = terms[0].astype(jnp.float32)
    for term in terms[1:]:
        total = total + term.astype(jnp.float32)
    return total


def await_bytes(ref, sem):
    pltpu.make_async_copy(ref, ref, sem).wait()


def kernel(
    n_z, n_grp, n_fsdp,
    grads, master_in, first_in, second_in,
    new_master, new_first, new_second, weights, copy_master, copy_first, copy_second,
    raw, other, own, early, part, late, flat, leaving, arriving, relayed, passing, passed, total, state,
    raw_sem, state_sem, other_sem, other_sent, early_sem, early_sent, late_sem, late_sent,
    far_sem, far_sent, relay_sem, pass_sem, pass_sent, weights_sem, weights_sent, copy_sem, copy_sent, known_sem,
):
    f, g = lax.axis_index("fsdp"), lax.axis_index("grp")
    z, y_lo = lax.rem(f, n_z), f // n_z
    core, x, y_hi = lax.rem(g, N_CORE), lax.rem(g // N_CORE, N_X), g // (N_CORE * N_X)
    y = y_hi * N_Y_LO + y_lo
    width = own.shape[-1]
    half = width // 2
    n_chunks = raw.shape[0]
    per_chunk = n_z // n_chunks

    def device(dx=0, dy=0, dz=0, flip=False):
        to_x, to_y = lax.rem(x + dx + N_X, N_X), lax.rem(y + dy + N_Y, N_Y)
        to_z = lax.rem(z + dz + n_z, n_z)
        to_core = 1 - core if flip else core
        return (
            lax.rem(to_y, N_Y_LO) * n_z + to_z,
            ((to_y // N_Y_LO) * N_X + to_x) * N_CORE + to_core,
        )

    def send(source, target, sent, received, to):
        pltpu.make_async_remote_copy(
            src_ref=source, dst_ref=target, send_sem=sent, recv_sem=received,
            device_id=to, device_id_type=MESH,
        ).start()

    def tell(sem, to):
        pl.semaphore_signal(sem, inc=1, device_id=to, device_id_type=MESH)

    def rows_of(to_y_hi):
        return slice(to_y_hi * N_Y_LO, (to_y_hi + 1) * N_Y_LO)

    def columns(to_y_hi, to_x, of_core):
        owner = (to_y_hi * N_X + to_x) * N_CORE + of_core
        return pl.ds(pl.multiple_of(owner * width, width), width)

    near = [
        device(flip=True), device(dx=1), device(dx=-1), device(dy=1), device(dy=-1),
        device(dz=1), device(dz=-1), device(dx=2), device(dy=2),
    ]
    def fetch(c):
        pltpu.make_async_copy(grads.at[:, c], raw.at[c], raw_sem.at[c]).start()

    fetch(0)
    barrier = pltpu.get_barrier_semaphore()
    for to in near:
        tell(barrier, to)

    first = jnp.logical_and(g == 0, y_lo == 0)
    later = jnp.logical_and(first, z != 0)
    root, helper = jnp.logical_and(first, z == 0), jnp.logical_and(first, z == 1)

    @pl.when(jnp.logical_and(z < GREETERS, jnp.logical_not(root)))
    def _():
        for d in range(1, n_z):
            tell(barrier, device(dz=d))

    for c in range(1, n_chunks):
        fetch(c)
    for i, source in enumerate((master_in, first_in, second_in)):
        pltpu.make_async_copy(source, state.at[i], state_sem).start()
    await_bytes(raw.at[0], raw_sem.at[0])
    greeted = jnp.where(z < GREETERS, GREETERS - 1, GREETERS) - jnp.where(later, 1, 0)
    pl.semaphore_wait(barrier, greeted + len(near))

    def exchange(c):
        if c:
            await_bytes(raw.at[c], raw_sem.at[c])
        for to_y_hi in range(N_Y_HI):
            for to_x in range(N_X):
                send(
                    raw.at[c, :, :, columns(to_y_hi, to_x, 1 - core)], other.at[c, rows_of(to_y_hi), to_x],
                    other_sent, other_sem.at[c], near[0],
                )

    n_known = known_sem.shape[0]

    def tell_far(i):
        for step in (1 << i, -(1 << i)):
            tell(known_sem.at[i], device(dz=step))

    def await_far(i):
        pl.semaphore_wait(known_sem.at[i], 2)
        if i + 1 < n_known:
            tell_far(i + 1)

    def both_cores(c):
        await_bytes(other.at[c], other_sem.at[c])
        for to_y_hi in range(N_Y_HI):
            for to_x in range(N_X):
                own[c, rows_of(to_y_hi), to_x] = add(
                    raw[c, :, :, columns(to_y_hi, to_x, core)], other[c, rows_of(to_y_hi), to_x]
                ).astype(own.dtype)
        for k in (2, 1, 3):
            to_x, to_y = lax.rem(x + k, N_X), lax.rem(y + k, N_Y)
            send(own.at[c, :, to_x, :, 0:half], early.at[c, 0, k - 1], early_sent, early_sem.at[c], device(dx=k))
            send(own.at[c, to_y, :, :, half:], early.at[c, 1, k - 1], early_sent, early_sem.at[c], device(dy=k))

    def second_axis(c):
        await_bytes(early.at[c], early_sem.at[c])
        for i in range(N_Y):
            part[c, 0, i] = add(own[c, i, x, :, 0:half], *[early[c, 0, k, i] for k in range(3)]).astype(part.dtype)
        for i in range(N_X):
            part[c, 1, i] = add(own[c, y, i, :, half:], *[early[c, 1, k, i] for k in range(3)]).astype(part.dtype)
        for k in (2, 1, 3):
            to_x, to_y = lax.rem(x + k, N_X), lax.rem(y + k, N_Y)
            send(part.at[c, 0, to_y], late.at[c, 0, k - 1], late_sent, late_sem.at[c], device(dy=k))
            send(part.at[c, 1, to_x], late.at[c, 1, k - 1], late_sent, late_sem.at[c], device(dx=k))

    def send_far(to_z, allowed):
        @pl.when(allowed)
        def _():
            d = lax.rem(to_z - z + n_z, n_z)
            send(leaving.at[to_z], arriving.at[d - 1], far_sent, far_sem, device(dz=d))

    def along_z(c):
        await_bytes(late.at[c], late_sem.at[c])
        ours = (part[c, 0, y], part[c, 1, x])
        tiles = width // LANES
        for a in range(2):
            plane = add(ours[a], *[late[c, a, k] for k in range(3)])
            for t in range(tiles // 2):
                flat[c, pl.ds(a * (tiles // 2) + t, CHUNK_ROWS, stride=tiles), :] = (
                    plane[:, t * LANES:(t + 1) * LANES]
                )
        leaving[c * per_chunk:(c + 1) * per_chunk] = (
            flat[c].reshape(per_chunk, *leaving.shape[1:]).astype(leaving.dtype)
        )
        for to_z in range(c * per_chunk, (c + 1) * per_chunk):
            allowed = z != to_z
            if to_z == 0:
                allowed = jnp.logical_and(allowed, jnp.logical_not(first))
            send_far(to_z, allowed)
        if c == 0:
            @pl.when(jnp.logical_and(first, z >= 2))
            def _():
                send(leaving.at[0], relayed.at[z - 2], far_sent, relay_sem, device(dz=1 - z))

    tell_far(0)
    steps = {"X": exchange, "E": both_cores, "Q": second_axis, "Z": along_z, "W": await_far}
    for step, i in ORDER:
        steps[step](i)

    await_bytes(state, state_sem)

    @pl.when(helper)
    def _():
        await_bytes(relayed, relay_sem)
        passing[...] = add(leaving[0], *[relayed[i] for i in range(n_z - 2)])
        send(passing, passed, pass_sent, pass_sem, device(dz=-1))

    @pl.when(root)
    def _():
        await_bytes(passed, pass_sem)
        total[...] = add(leaving[0], passed[...])

    @pl.when(jnp.logical_not(root))
    def _():
        await_bytes(arriving, far_sem)
        total[...] = add(leaving[z], *[arriving[d] for d in range(n_z - 1)])

    scale = 1.0 / (n_grp * n_fsdp)
    for t in range(width // LANES):
        at = slice(t * LANES, (t + 1) * LANES)
        gradient = total[pl.ds(t, 2, stride=width // LANES), :] * scale
        one = beta_one * state[1, :, at] + (1.0 - beta_one) * gradient
        two = beta_two * state[2, :, at] + (1.0 - beta_two) * gradient * gradient
        one_hat = one / (1.0 - beta_one**step_count)
        two_hat = two / (1.0 - beta_two**step_count)
        old = state[0, :, at]
        new = old - learn_rate * (one_hat / (jnp.sqrt(two_hat) + epsilon) + decay_rate * old)
        new_master[:, at] = new
        new_first[:, at] = one
        new_second[:, at] = two
    mine = pl.ds(pl.multiple_of(g * width, width), width)
    weights[:, mine] = new_master[...].astype(weights.dtype)
    after = (f, lax.rem(g + 1, n_grp))
    for i in range(n_grp - 1, 0, -1):
        to = lax.rem(g + i, n_grp)
        send(weights.at[:, mine], weights.at[:, mine], weights_sent, weights_sem, (f, to))
    copies = ((new_master, copy_master), (new_first, copy_first), (new_second, copy_second))
    for new, copied in copies:
        send(new, copied, copy_sent, copy_sem, after)

    await_bytes(other, other_sent)
    await_bytes(early, early_sent)
    await_bytes(late, late_sent)


    @pl.when(helper)
    def _():
        await_bytes(arriving.at[1:], far_sent)
        await_bytes(passing, pass_sent)

    @pl.when(jnp.logical_not(helper))
    def _():
        await_bytes(arriving, far_sent)

    others = weights.at[:, 0:(n_grp - 1) * width]
    await_bytes(others, weights_sem)
    await_bytes(others, weights_sent)
    await_bytes(state, copy_sem)
    await_bytes(state, copy_sent)


def put_out(*refs):
    n = len(refs) // 2
    sem = refs[-1]
    copies = [pltpu.make_async_copy(refs[i], refs[n + i], sem.at[i]) for i in range(n)]
    for copy in copies:
        copy.start()
    for copy in copies:
        copy.wait()


def shards(n_fsdp, n_grp, grads, master, moment_one, moment_two):
    rows, columns = grads.shape[2:]
    n_z = n_fsdp // N_Y_LO
    width = columns // n_grp
    half = width // 2
    n_chunks = rows // (N_Y_LO * CHUNK_ROWS)
    piece = (rows // n_fsdp) * width // LANES
    vmem = pl.BlockSpec(memory_space=pltpu.VMEM)
    hbm = pl.BlockSpec(memory_space=pltpu.HBM)
    small = jax.ShapeDtypeStruct(master.shape, jnp.float32)
    wide = jax.ShapeDtypeStruct((master.shape[0], columns), jnp.bfloat16)
    outputs = (small, small, small, wide, small, small, small)
    bf16, f32, dma = jnp.bfloat16, jnp.float32, pltpu.SemaphoreType.DMA
    r = CHUNK_ROWS
    results = pl.pallas_call(
        functools.partial(kernel, n_z, n_grp, n_fsdp),
        out_shape=[pltpu.VMEM(o.shape, o.dtype) for o in outputs],
        in_specs=[hbm] * 4,
        out_specs=[vmem] * 7,
        scratch_shapes=[
            pltpu.VMEM((n_chunks, N_Y_LO, r, columns), bf16),
            pltpu.VMEM((n_chunks, N_Y, N_X, r, width), bf16),
            pltpu.VMEM((n_chunks, N_Y, N_X, r, width), bf16),
            pltpu.VMEM((n_chunks, 2, 3, N_X, r, half), bf16),
            pltpu.VMEM((n_chunks, 2, N_X, r, half), bf16),
            pltpu.VMEM((n_chunks, 2, 3, r, half), bf16),
            pltpu.VMEM((n_chunks, r * width // LANES, LANES), f32),
            pltpu.VMEM((n_z, piece, LANES), bf16),
            pltpu.VMEM((n_z - 1, piece, LANES), bf16),
            pltpu.VMEM((n_z - 2, piece, LANES), bf16),
            pltpu.VMEM((piece, LANES), f32), pltpu.VMEM((piece, LANES), f32), pltpu.VMEM((piece, LANES), f32),
            pltpu.VMEM((3, *master.shape), f32),
            dma((n_chunks,)), dma, dma((n_chunks,)), dma,
            dma((n_chunks,)), dma, dma((n_chunks,)), dma,
            dma, dma, dma, dma, dma,
            dma, dma, dma, dma,
            pltpu.SemaphoreType.REGULAR((n_z.bit_length() - 2,)),
        ],
        compiler_params=pltpu.CompilerParams(
            collective_id=0, has_side_effects=True, vmem_limit_bytes=16 << 20
        ),
        name="step",
    )(*[
        pltpu.with_memory_space_constraint(a, pltpu.HBM)
        for a in (grads.reshape(N_Y_LO, n_chunks, r, columns), master, moment_one, moment_two)
    ])
    return pl.pallas_call(
        put_out,
        out_shape=outputs,
        in_specs=[vmem] * 7,
        out_specs=[pl.BlockSpec(memory_space=pltpu.HBM)] * 7,
        scratch_shapes=[dma((7,))],
        compiler_params=pltpu.CompilerParams(vmem_limit_bytes=1 << 20),
        name="put_out",
    )(*results)


def solution(mesh):
    return jax.shard_map(
        functools.partial(shards, mesh.shape["fsdp"], mesh.shape["grp"]),
        mesh=mesh,
        in_specs=(P("grp", "fsdp", None, None), P("fsdp", "grp"), P("fsdp", "grp"), P("fsdp", "grp")),
        out_specs=(
            P("fsdp", "grp"), P("fsdp", "grp"), P("fsdp", "grp"), P("fsdp", None),
            P("fsdp", "grp"), P("fsdp", "grp"), P("fsdp", "grp"),
        ),
        check_vma=False,
    )
```
